32 devices in a mesh: ep: 32 (over z, y, x, core).
Axes of the slice: x: 2, y: 2, z: 4, core: 2. Of those that a mesh axis runs over, the one named last changes fastest.
Arguments:
- x_tokens: bfloat16 [131072, 768], P('ep')
- w_router: float32 [768, 32], replicated
- expert_idx: int32 [131072], P('ep')
- w_in: bfloat16 [32, 768, 3072], P('ep')
- w_out: bfloat16 [32, 3072, 768], P('ep')
- grad_y: bfloat16 [131072, 768], P('ep')
Outputs:
- output 1: bfloat16 [131072, 768], P('ep')
- output 2: float32 [32, 768, 3072], P('ep')
- output 3: float32 [32, 3072, 768], P('ep')
- output 4: float32 [768, 32], replicated
- output 5: float32 [], replicated
- output 6: float32 [], replicated
All inputs are finite; a program needn't handle non-finite values.
Results may differ from the reference program's by a relative error of at most 0.012471.
Values are sent between devices in bfloat16 or wider.
A program may use at most 1 GiB of HBM per device.

```python
import jax
import jax.numpy as jnp
from jax import lax

D = 768
FF = 3072
EXPERTS = 32
TOKENS = 4096
GROUPS = 32

CAPACITY = (5 * TOKENS + 4 * EXPERTS - 1) // (4 * EXPERTS)
TOTAL_TOK = GROUPS * TOKENS
N_SLOTS = EXPERTS * CAPACITY
AUX_WEIGHT = 0.01
Z_WEIGHT = 0.001
LOGIT_SCALE = 1.5


def draw_routes(route_key):
    key_perm, key_hot, key_tok = jax.random.split(route_key, 3)
    expert_perm = jax.random.permutation(key_perm, EXPERTS)
    hot_expert = jax.random.randint(key_hot, (GROUPS,), 0, EXPERTS)
    n_hot = TOKENS // 4
    n_rest = TOKENS - n_hot - EXPERTS

    def one_group(group_id):
        key_a, key_b, key_c = jax.random.split(jax.random.fold_in(key_tok, group_id), 3)
        first_pick = jax.random.randint(key_a, (n_rest,), 0, EXPERTS)
        second_pick = jax.random.randint(key_b, (n_rest,), 0, EXPERTS)
        skewed = expert_perm[jnp.minimum(first_pick, second_pick)].astype(jnp.int32)
        hot_rows = jnp.full((n_hot,), hot_expert[group_id], jnp.int32)
        listed = jnp.concatenate([hot_rows, jnp.arange(EXPERTS, dtype=jnp.int32), skewed])
        return listed[jax.random.permutation(key_c, TOKENS)]

    return jax.vmap(one_group)(jnp.arange(GROUPS)).reshape(TOTAL_TOK).astype(jnp.int32)


def setup_inputs(seed: int = 0) -> dict:
    base_key = jax.random.key(seed)
    key_x, key_router, key_in, key_out, key_gy, key_route = jax.random.split(base_key, 6)
    x_tokens = jax.random.normal(key_x, (TOTAL_TOK, D), jnp.float32).astype(jnp.bfloat16)
    w_router = jax.random.normal(key_router, (D, EXPERTS), jnp.float32) * (LOGIT_SCALE * D ** -0.5)
    w_in = (jax.random.normal(key_in, (EXPERTS, D, FF), jnp.float32) * D ** -0.5).astype(jnp.bfloat16)
    w_out = (jax.random.normal(key_out, (EXPERTS, FF, D), jnp.float32) * FF ** -0.5).astype(jnp.bfloat16)
    grad_y = jax.random.normal(key_gy, (TOTAL_TOK, D), jnp.float32).astype(jnp.bfloat16)
    expert_idx = draw_routes(key_route)
    return {'x_tokens': x_tokens, 'w_router': w_router, 'expert_idx': expert_idx, 'w_in': w_in, 'w_out': w_out, 'grad_y': grad_y}


def router_group(x_group, w_router, idx_group):
    logits = jnp.dot(x_group.astype(jnp.float32), w_router)
    router_prob = jax.nn.softmax(logits, axis=-1)
    log_norm = jax.nn.logsumexp(logits, axis=-1)
    onehot = (idx_group[:, None] == jnp.arange(EXPERTS)[None, :]).astype(jnp.int32)
    position = jnp.sum(jnp.cumsum(onehot, axis=0) * onehot, axis=1) - 1
    tok_slot = jnp.where(position < CAPACITY, idx_group * CAPACITY + position, N_SLOTS)
    onehot_f = onehot.astype(jnp.float32)
    gate_val = jnp.sum(router_prob * onehot_f, axis=-1)
    return router_prob, log_norm, onehot_f, gate_val, tok_slot


def reference(x_tokens, w_router, expert_idx, w_in, w_out, grad_y):
    x_groups = x_tokens.reshape(GROUPS, TOKENS, D)
    idx_groups = expert_idx.reshape(GROUPS, TOKENS)
    gy_groups = grad_y.reshape(GROUPS, TOKENS, D)

    def first_pass(operands):
        x_group, idx_group, gy_group = operands
        router_prob, log_norm, onehot_f, gate_val, tok_slot = router_group(x_group, w_router, idx_group)
        scaled = (gate_val[:, None] * gy_group.astype(jnp.float32)).astype(jnp.bfloat16)
        empty_buf = jnp.zeros((N_SLOTS + 1, D), jnp.bfloat16)
        sent_rows = empty_buf.at[tok_slot].set(x_group)[:N_SLOTS]
        sent_grad = empty_buf.at[tok_slot].set(scaled)[:N_SLOTS]
        route_stats = jnp.concatenate([jnp.sum(onehot_f, axis=0), jnp.sum(router_prob, axis=0), jnp.sum(log_norm * log_norm)[None]])
        return sent_rows, sent_grad, route_stats

    sent_rows, sent_grad, route_stats = lax.map(first_pass, (x_groups, idx_groups, gy_groups))
    rows_all = sent_rows.reshape(GROUPS, EXPERTS, CAPACITY, D).transpose(1, 0, 2, 3).reshape(EXPERTS, GROUPS * CAPACITY, D)
    grads_all = sent_grad.reshape(GROUPS, EXPERTS, CAPACITY, D).transpose(1, 0, 2, 3).reshape(EXPERTS, GROUPS * CAPACITY, D)

    def expert_pass(operands):
        recv_rows, recv_grad, w_first, w_second = operands
        pre_act = jnp.dot(recv_rows, w_first, preferred_element_type=jnp.float32)
        hidden = jnp.maximum(pre_act, 0.0).astype(jnp.bfloat16)
        expert_out = jnp.dot(hidden, w_second, preferred_element_type=jnp.float32).astype(jnp.bfloat16)
        d_hidden = jnp.dot(recv_grad, w_second.T, preferred_element_type=jnp.float32)
        d_pre = jnp.where(hidden > 0, d_hidden, 0.0).astype(jnp.bfloat16)
        grad_out_e = jnp.dot(hidden.T, recv_grad, preferred_element_type=jnp.float32)
        grad_in_e = jnp.dot(recv_rows.T, d_pre, preferred_element_type=jnp.float32)
        d_rows = jnp.dot(d_pre, w_first.T, preferred_element_type=jnp.float32).astype(jnp.bfloat16)
        return expert_out, d_rows, grad_in_e, grad_out_e

    expert_out, d_rows, grad_w_in, grad_w_out = lax.map(expert_pass, (rows_all, grads_all, w_in, w_out))
    out_groups = expert_out.reshape(EXPERTS, GROUPS, CAPACITY, D).transpose(1, 0, 2, 3).reshape(GROUPS, N_SLOTS, D)
    back_groups = d_rows.reshape(EXPERTS, GROUPS, CAPACITY, D).transpose(1, 0, 2, 3).reshape(GROUPS, N_SLOTS, D)

    totals = jnp.sum(route_stats, axis=0)
    load_frac = totals[:EXPERTS] / TOTAL_TOK
    mean_prob = totals[EXPERTS:2 * EXPERTS] / TOTAL_TOK
    aux_loss = AUX_WEIGHT * EXPERTS * jnp.sum(load_frac * mean_prob)
    z_loss = Z_WEIGHT * totals[2 * EXPERTS] / TOTAL_TOK
    aux_vec = AUX_WEIGHT * EXPERTS * load_frac / TOTAL_TOK
    z_coef = 2.0 * Z_WEIGHT / TOTAL_TOK
    pad_row = jnp.zeros((1, D), jnp.bfloat16)

    def second_pass(operands):
        x_group, idx_group, gy_group, out_group, back_group = operands
        router_prob, log_norm, onehot_f, gate_val, tok_slot = router_group(x_group, w_router, idx_group)
        out_tok = jnp.concatenate([out_group, pad_row])[tok_slot]
        back_tok = jnp.concatenate([back_group, pad_row])[tok_slot]
        d_gate = jnp.sum(out_tok.astype(jnp.float32) * gy_group.astype(jnp.float32), axis=-1)
        spread = jnp.sum(router_prob * aux_vec[None, :], axis=-1, keepdims=True)
        d_logits = ((gate_val * d_gate)[:, None] * (onehot_f - router_prob)
                    + router_prob * (aux_vec[None, :] - spread)
                    + (z_coef * log_norm)[:, None] * router_prob)
        grad_x = (back_tok.astype(jnp.float32) + jnp.dot(d_logits, w_router.T)).astype(jnp.bfloat16)
        part_router = jnp.dot(x_group.astype(jnp.float32).T, d_logits)
        return grad_x, part_router

    grad_x, parts_router = lax.map(second_pass, (x_groups, idx_groups, gy_groups, out_groups, back_groups))
    return grad_x.reshape(TOTAL_TOK, D), grad_w_in, grad_w_out, jnp.sum(parts_router, axis=0), aux_loss, z_loss
```

```python
import jax
import jax.numpy as jnp
from jax import lax
from jax.sharding import PartitionSpec as P

AUX_WEIGHT = 0.01
Z_WEIGHT = 0.001
CHUNKS = 2
BLOCK = 256
BF = jnp.bfloat16
F32 = jnp.float32


def route(idx, num_experts, capacity):
    tokens = idx.shape[0]
    hot = (idx[:, None] == jnp.arange(num_experts, dtype=jnp.int32)[None, :]).astype(BF)
    blocks = hot.reshape(tokens // BLOCK, BLOCK, num_experts)
    row = lax.broadcasted_iota(jnp.int32, (BLOCK, BLOCK), 0)
    col = lax.broadcasted_iota(jnp.int32, (BLOCK, BLOCK), 1)
    inside = jnp.einsum('ij,bje->bie', (col <= row).astype(BF), blocks, preferred_element_type=F32)
    totals = inside[:, -1, :]
    n_blocks = tokens // BLOCK
    earlier = (jnp.arange(n_blocks)[None, :] < jnp.arange(n_blocks)[:, None]).astype(F32)
    before = jnp.sum(earlier[:, :, None] * totals[None, :, :], axis=1)
    counts = (before[-1] + totals[-1]).astype(jnp.int32)
    position = jnp.sum((inside + before[:, None, :]) * blocks.astype(F32), axis=-1).reshape(tokens).astype(jnp.int32) - 1
    pos_hot = (position[:, None] == jnp.arange(capacity, dtype=jnp.int32)[None, :]).astype(BF)
    token = jnp.arange(tokens, dtype=jnp.int32)
    parts = jnp.concatenate([hot * (token // 64).astype(BF)[:, None], hot * (token % 64).astype(BF)[:, None]], axis=1)
    found = jnp.einsum('te,tp->ep', parts, pos_hot, preferred_element_type=F32)
    slot_tok = (64.0 * found[:num_experts] + found[num_experts:]).astype(jnp.int32)
    return hot, pos_hot, counts, position, slot_tok


def rows_of(source, index):
    return source.at[index].get(mode='promise_in_bounds')


def router(rows, w_router):
    logits = jnp.dot(rows, w_router, preferred_element_type=F32)
    return jax.nn.softmax(logits, axis=-1), jax.nn.logsumexp(logits, axis=-1)


def solution(mesh):
    n_dev = mesh.shape['ep']

    def expert_layer(x_tokens, w_router, expert_idx, w_in, w_out, grad_y):
        tokens, d_model = x_tokens.shape
        num_experts = n_dev
        capacity = (5 * tokens + 4 * num_experts - 1) // (4 * num_experts)
        total_tok = tokens * n_dev
        width = capacity // CHUNKS
        me = lax.axis_index('ep')
        w_in, w_out = w_in[0], w_out[0]

        def exchange(rows):
            return lax.all_to_all(rows, 'ep', 0, 0, tiled=True)

        hot, pos_hot, counts, position, slot_tok = route(expert_idx, num_experts, capacity)
        hot_f = hot.astype(F32)
        all_counts = exchange(jnp.broadcast_to(counts[None, :], (n_dev, num_experts)))
        arriving = lax.dynamic_index_in_dim(all_counts, me, 1, keepdims=False)
        load_frac = jnp.sum(all_counts, axis=0).astype(F32) / total_tok

        n_rows = n_dev * width
        first = slot_tok[:, :width]
        second = slot_tok[:, width:]

        def picked(source, index):
            return rows_of(source, index.reshape(-1)).reshape(n_dev, index.shape[1], d_model)

        x_first = exchange(picked(x_tokens, first)).reshape(n_rows, d_model)
        both = jnp.concatenate([grad_y, x_tokens], axis=0)
        middle = exchange(picked(both, jnp.concatenate([first, second + tokens], axis=1)))
        dy_last, middle = lax.optimization_barrier((picked(grad_y, second), middle))
        dy_last = exchange(dy_last).reshape(n_rows, d_model)
        dy_first = middle[:, :width].reshape(n_rows, d_model)
        x_last = middle[:, width:].reshape(n_rows, d_model)

        prob, log_norm = router(x_tokens, w_router)
        gate = jnp.sum(prob * hot_f, axis=-1)
        aux_vec = AUX_WEIGHT * num_experts * load_frac / total_tok
        spread = jnp.sum(prob * aux_vec, axis=-1, keepdims=True)
        d_logits = prob * (aux_vec - spread) + (2.0 * Z_WEIGHT / total_tok * log_norm)[:, None] * prob
        part_router = jnp.einsum('sd,se->de', x_tokens, d_logits, preferred_element_type=F32)

        mine = (jnp.arange(num_experts) == me).astype(F32)[None, :]

        def forward(j, rows, dy):
            slot_prob, _ = router(rows, w_router)
            slot_gate = jnp.sum(slot_prob * mine, axis=-1)
            hidden = jnp.maximum(jnp.dot(rows, w_in, preferred_element_type=F32), 0.0).astype(BF)
            expert_out = jnp.dot(hidden, w_out, preferred_element_type=F32).astype(BF)
            dy_f = dy.astype(F32)
            slots = j * width + jnp.arange(width, dtype=jnp.int32)
            valid = (slots[None, :] < arriving[:, None]).reshape(n_rows)
            slot_dot = jnp.where(valid, jnp.sum(expert_out.astype(F32) * dy_f, axis=-1), 0.0)
            scaled = jnp.where(valid[:, None], slot_gate[:, None] * dy_f, 0.0).astype(BF)
            slot_logits = (slot_gate * slot_dot)[:, None] * (mine - slot_prob)
            part = jnp.einsum('sd,se->de', rows, slot_logits, preferred_element_type=F32)
            return hidden, scaled, slot_dot.reshape(n_dev, width), part

        def backward(hidden, scaled):
            d_hidden = jnp.einsum('nd,fd->nf', scaled, w_out, preferred_element_type=F32)
            d_pre = jnp.where(hidden > 0, d_hidden, 0.0).astype(BF)
            d_rows = jnp.einsum('nf,df->nd', d_pre, w_in, preferred_element_type=F32).astype(BF)
            return d_pre, d_rows.reshape(n_dev, width, d_model)

        def weights(rows, hidden, scaled, d_pre):
            return (jnp.einsum('nd,nf->df', rows, d_pre, preferred_element_type=F32),
                    jnp.einsum('nf,nd->fd', hidden, scaled, preferred_element_type=F32))

        hidden_a, scaled_a, dot_a, part_a = forward(0, x_first, dy_first)
        pre_a, d_rows_a = backward(hidden_a, scaled_a)
        back_a = exchange(d_rows_a)
        hidden_b, scaled_b, dot_b, part_b = forward(1, x_last, dy_last)
        pre_b, d_rows_b = backward(hidden_b, scaled_b)

        part_router += part_a + part_b
        slices = part_router.reshape(n_dev, -1)
        prob_sum = jnp.sum(prob, axis=0)[:, None]
        z_sum = jnp.full((n_dev, 1), jnp.sum(log_norm * log_norm))
        payload = jnp.concatenate([dot_a, dot_b, slices, prob_sum, z_sum], axis=1)
        payload, back_a, d_rows_b = lax.optimization_barrier((payload, back_a, d_rows_b))
        payload = exchange(payload)
        payload, d_rows_b = lax.optimization_barrier((payload, d_rows_b))
        back_b = exchange(d_rows_b)
        reduced = jnp.sum(payload[:, capacity:], axis=0)
        reduced, back_b = lax.optimization_barrier((reduced, back_b))
        totals = exchange(jnp.broadcast_to(reduced[None, :], (n_dev, reduced.shape[0])))
        grad_w_router = totals[:, :-2].reshape(d_model, num_experts)
        aux_loss = AUX_WEIGHT * num_experts * jnp.sum(load_frac * (totals[:, -2] / total_tok))
        z_loss = Z_WEIGHT * totals[0, -1] / total_tok

        payload, hidden_a, pre_a, back_a = lax.optimization_barrier((payload, hidden_a, pre_a, back_a))
        in_a, out_a = weights(x_first, hidden_a, scaled_a, pre_a)
        in_b, out_b = weights(x_last, hidden_b, scaled_b, pre_b)

        all_dot = payload[:, :capacity]
        spread_dot = jnp.dot(hot_f, all_dot, precision=lax.Precision.HIGHEST, preferred_element_type=F32)
        d_gate = jnp.sum(jnp.where(pos_hot > 0, spread_dot, 0.0), axis=-1)
        d_logits += (gate * d_gate)[:, None] * (hot_f - prob)
        dx = jnp.einsum('se,de->sd', d_logits, w_router)
        for j, back in enumerate((back_a, back_b)):
            inside = position - j * width
            index = expert_idx * width + jnp.clip(inside, 0, width - 1)
            held = (inside >= 0) & (inside < width)
            dx += jnp.where(held[:, None], rows_of(back.reshape(n_rows, d_model), index).astype(F32), 0.0)
        return dx.astype(BF), (in_a + in_b)[None], (out_a + out_b)[None], grad_w_router, aux_loss, z_loss

    return jax.shard_map(expert_layer, mesh=mesh,
                         in_specs=(P('ep', None), P(None, None), P('ep'), P('ep', None, None), P('ep', None, None), P('ep', None)),
                         out_specs=(P('ep', None), P('ep', None, None), P('ep', None, None), P(None, None), P(), P()),
                         check_vma=False)
```

```python
import jax
import jax.numpy as jnp
from jax import lax
from jax.sharding import PartitionSpec as P

AUX_WEIGHT = 0.01
Z_WEIGHT = 0.001
CHUNKS = 2
BLOCK = 256
BF = jnp.bfloat16
F32 = jnp.float32


def route(idx, num_experts, capacity):
    tokens = idx.shape[0]
    hot = (idx[:, None] == jnp.arange(num_experts, dtype=jnp.int32)[None, :]).astype(BF)
    blocks = hot.reshape(tokens // BLOCK, BLOCK, num_experts)
    row = lax.broadcasted_iota(jnp.int32, (BLOCK, BLOCK), 0)
    col = lax.broadcasted_iota(jnp.int32, (BLOCK, BLOCK), 1)
    inside = jnp.einsum('ij,bje->bie', (col <= row).astype(BF), blocks, preferred_element_type=F32)
    totals = inside[:, -1, :]
    n_blocks = tokens // BLOCK
    earlier = (jnp.arange(n_blocks)[None, :] < jnp.arange(n_blocks)[:, None]).astype(F32)
    before = jnp.sum(earlier[:, :, None] * totals[None, :, :], axis=1)
    counts = (before[-1] + totals[-1]).astype(jnp.int32)
    position = jnp.sum((inside + before[:, None, :]) * blocks.astype(F32), axis=-1).reshape(tokens).astype(jnp.int32) - 1
    pos_hot = (position[:, None] == jnp.arange(capacity, dtype=jnp.int32)[None, :]).astype(BF)
    token = jnp.arange(tokens, dtype=jnp.int32)
    parts = jnp.concatenate([hot * (token // 64).astype(BF)[:, None], hot * (token % 64).astype(BF)[:, None]], axis=1)
    found = jnp.einsum('te,tp->ep', parts, pos_hot, preferred_element_type=F32)
    slot_tok = (64.0 * found[:num_experts] + found[num_experts:]).astype(jnp.int32)
    return hot, pos_hot, counts, position, slot_tok


def rows_of(source, index):
    return source.at[index].get(mode='promise_in_bounds')


def router(rows, w_router):
    logits = jnp.dot(rows, w_router, preferred_element_type=F32)
    return jax.nn.softmax(logits, axis=-1), jax.nn.logsumexp(logits, axis=-1)


def solution(mesh):
    n_dev = mesh.shape['ep']

    def expert_layer(x_tokens, w_router, expert_idx, w_in, w_out, grad_y):
        tokens, d_model = x_tokens.shape
        num_experts = n_dev
        capacity = (5 * tokens + 4 * num_experts - 1) // (4 * num_experts)
        total_tok = tokens * n_dev
        width = capacity // CHUNKS
        me = lax.axis_index('ep')
        w_in, w_out = w_in[0], w_out[0]

        def exchange(rows):
            return lax.all_to_all(rows, 'ep', 0, 0, tiled=True)

        hot, pos_hot, counts, position, slot_tok = route(expert_idx, num_experts, capacity)
        hot_f = hot.astype(F32)
        all_counts = exchange(jnp.broadcast_to(counts[None, :], (n_dev, num_experts)))

        n_rows = n_dev * width
        first = slot_tok[:, :width]
        second = slot_tok[:, width:]

        def picked(source, index):
            return rows_of(source, index.reshape(-1)).reshape(n_dev, index.shape[1], d_model)

        x_first, all_counts = lax.optimization_barrier((picked(x_tokens, first), all_counts))
        x_first = exchange(x_first).reshape(n_rows, d_model)
        arriving = lax.dynamic_index_in_dim(all_counts, me, 1, keepdims=False)
        load_frac = jnp.sum(all_counts, axis=0).astype(F32) / total_tok
        dy_first, x_first = lax.optimization_barrier((picked(grad_y, first), x_first))
        dy_first = exchange(dy_first).reshape(n_rows, d_model)
        x_last, dy_first = lax.optimization_barrier((picked(x_tokens, second), dy_first))
        x_last = exchange(x_last).reshape(n_rows, d_model)
        dy_last, x_last = lax.optimization_barrier((picked(grad_y, second), x_last))
        dy_last = exchange(dy_last).reshape(n_rows, d_model)

        prob, log_norm = router(x_tokens, w_router)
        gate = jnp.sum(prob * hot_f, axis=-1)
        aux_vec = AUX_WEIGHT * num_experts * load_frac / total_tok
        spread = jnp.sum(prob * aux_vec, axis=-1, keepdims=True)
        d_logits = prob * (aux_vec - spread) + (2.0 * Z_WEIGHT / total_tok * log_norm)[:, None] * prob
        part_router = jnp.einsum('sd,se->de', x_tokens, d_logits, preferred_element_type=F32)

        mine = (jnp.arange(num_experts) == me).astype(F32)[None, :]

        def forward(j, rows, dy):
            slot_prob, _ = router(rows, w_router)
            slot_gate = jnp.sum(slot_prob * mine, axis=-1)
            hidden = jnp.maximum(jnp.dot(rows, w_in, preferred_element_type=F32), 0.0).astype(BF)
            expert_out = jnp.dot(hidden, w_out, preferred_element_type=F32).astype(BF)
            dy_f = dy.astype(F32)
            slots = j * width + jnp.arange(width, dtype=jnp.int32)
            valid = (slots[None, :] < arriving[:, None]).reshape(n_rows)
            slot_dot = jnp.where(valid, jnp.sum(expert_out.astype(F32) * dy_f, axis=-1), 0.0)
            scaled = jnp.where(valid[:, None], slot_gate[:, None] * dy_f, 0.0).astype(BF)
            slot_logits = (slot_gate * slot_dot)[:, None] * (mine - slot_prob)
            part = jnp.einsum('sd,se->de', rows, slot_logits, preferred_element_type=F32)
            return hidden, scaled, slot_dot.reshape(n_dev, width), part

        def backward(hidden, scaled):
            d_hidden = jnp.einsum('nd,fd->nf', scaled, w_out, preferred_element_type=F32)
            d_pre = jnp.where(hidden > 0, d_hidden, 0.0).astype(BF)
            d_rows = jnp.einsum('nf,df->nd', d_pre, w_in, preferred_element_type=F32).astype(BF)
            return d_pre, d_rows.reshape(n_dev, width, d_model)

        def weights(rows, hidden, scaled, d_pre):
            return (jnp.einsum('nd,nf->df', rows, d_pre, preferred_element_type=F32),
                    jnp.einsum('nf,nd->fd', hidden, scaled, preferred_element_type=F32))

        hidden_a, scaled_a, dot_a, part_a = forward(0, x_first, dy_first)
        pre_a, d_rows_a = backward(hidden_a, scaled_a)
        in_a, out_a = weights(x_first, hidden_a, scaled_a, pre_a)
        d_rows_a, in_a, out_a = lax.optimization_barrier((d_rows_a, in_a, out_a))
        back_a = exchange(d_rows_a)
        hidden_b, scaled_b, dot_b, part_b = forward(1, x_last, dy_last)
        pre_b, d_rows_b = backward(hidden_b, scaled_b)

        part_router += part_a + part_b
        slices = part_router.reshape(n_dev, -1)
        prob_sum = jnp.sum(prob, axis=0)[:, None]
        z_sum = jnp.full((n_dev, 1), jnp.sum(log_norm * log_norm))
        payload = jnp.concatenate([dot_a, dot_b, slices, prob_sum, z_sum], axis=1)
        payload, back_a, d_rows_b = lax.optimization_barrier((payload, back_a, d_rows_b))
        payload = exchange(payload)
        payload, d_rows_b = lax.optimization_barrier((payload, d_rows_b))
        back_b = exchange(d_rows_b)
        reduced = jnp.sum(payload[:, capacity:], axis=0)
        reduced, back_b = lax.optimization_barrier((reduced, back_b))
        totals = exchange(jnp.broadcast_to(reduced[None, :], (n_dev, reduced.shape[0])))
        grad_w_router = totals[:, :-2].reshape(d_model, num_experts)
        aux_loss = AUX_WEIGHT * num_experts * jnp.sum(load_frac * (totals[:, -2] / total_tok))
        z_loss = Z_WEIGHT * totals[0, -1] / total_tok

        payload, hidden_b, pre_b, back_a = lax.optimization_barrier((payload, hidden_b, pre_b, back_a))
        in_b, out_b = weights(x_last, hidden_b, scaled_b, pre_b)

        all_dot = payload[:, :capacity]
        spread_dot = jnp.dot(hot_f, all_dot, precision=lax.Precision.HIGHEST, preferred_element_type=F32)
        d_gate = jnp.sum(jnp.where(pos_hot > 0, spread_dot, 0.0), axis=-1)
        d_logits += (gate * d_gate)[:, None] * (hot_f - prob)
        dx = jnp.einsum('se,de->sd', d_logits, w_router)
        for j, back in enumerate((back_a, back_b)):
            inside = position - j * width
            index = expert_idx * width + jnp.clip(inside, 0, width - 1)
            held = (inside >= 0) & (inside < width)
            dx += jnp.where(held[:, None], rows_of(back.reshape(n_rows, d_model), index).astype(F32), 0.0)
        return dx.astype(BF), (in_a + in_b)[None], (out_a + out_b)[None], grad_w_router, aux_loss, z_loss

    return jax.shard_map(expert_layer, mesh=mesh,
                         in_specs=(P('ep', None), P(None, None), P('ep'), P('ep', None, None), P('ep', None, None), P('ep', None)),
                         out_specs=(P('ep', None), P('ep', None, None), P('ep', None, None), P(None, None), P(), P()),
                         check_vma=False)
```

```python
import jax
import jax.numpy as jnp
from jax import lax
from jax.sharding import PartitionSpec as P

AUX_WEIGHT = 0.01
Z_WEIGHT = 0.001
CHUNKS = 2
BLOCK = 256
BF = jnp.bfloat16
F32 = jnp.float32


def route(idx, num_experts, capacity):
    tokens = idx.shape[0]
    hot = (idx[:, None] == jnp.arange(num_experts, dtype=jnp.int32)[None, :]).astype(BF)
    blocks = hot.reshape(tokens // BLOCK, BLOCK, num_experts)
    row = lax.broadcasted_iota(jnp.int32, (BLOCK, BLOCK), 0)
    col = lax.broadcasted_iota(jnp.int32, (BLOCK, BLOCK), 1)
    inside = jnp.einsum('ij,bje->bie', (col <= row).astype(BF), blocks, preferred_element_type=F32)
    totals = inside[:, -1, :]
    n_blocks = tokens // BLOCK
    earlier = (jnp.arange(n_blocks)[None, :] < jnp.arange(n_blocks)[:, None]).astype(F32)
    before = jnp.sum(earlier[:, :, None] * totals[None, :, :], axis=1)
    counts = (before[-1] + totals[-1]).astype(jnp.int32)
    position = jnp.sum((inside + before[:, None, :]) * blocks.astype(F32), axis=-1).reshape(tokens).astype(jnp.int32) - 1
    pos_hot = (position[:, None] == jnp.arange(capacity, dtype=jnp.int32)[None, :]).astype(BF)
    token = jnp.arange(tokens, dtype=jnp.int32)
    parts = jnp.concatenate([hot * (token // 64).astype(BF)[:, None], hot * (token % 64).astype(BF)[:, None]], axis=1)
    found = jnp.einsum('te,tp->ep', parts, pos_hot, preferred_element_type=F32)
    slot_tok = (64.0 * found[:num_experts] + found[num_experts:]).astype(jnp.int32)
    return hot, pos_hot, counts, position, slot_tok


def rows_of(source, index):
    return source.at[index].get(mode='promise_in_bounds')


def router(rows, w_router):
    logits = jnp.dot(rows, w_router, preferred_element_type=F32)
    return jax.nn.softmax(logits, axis=-1), jax.nn.logsumexp(logits, axis=-1)


def solution(mesh):
    n_dev = mesh.shape['ep']

    def expert_layer(x_tokens, w_router, expert_idx, w_in, w_out, grad_y):
        tokens, d_model = x_tokens.shape
        num_experts = n_dev
        capacity = (5 * tokens + 4 * num_experts - 1) // (4 * num_experts)
        total_tok = tokens * n_dev
        width = capacity // CHUNKS
        me = lax.axis_index('ep')
        w_in, w_out = w_in[0], w_out[0]

        def exchange(rows):
            return lax.all_to_all(rows, 'ep', 0, 0, tiled=True)

        hot, pos_hot, counts, position, slot_tok = route(expert_idx, num_experts, capacity)
        hot_f = hot.astype(F32)
        all_counts = exchange(jnp.broadcast_to(counts[None, :], (n_dev, num_experts)))

        n_rows = n_dev * width
        first = slot_tok[:, :width]
        second = slot_tok[:, width:]

        def picked(source, index):
            return rows_of(source, index.reshape(-1)).reshape(n_dev, index.shape[1], d_model)

        x_first, all_counts = lax.optimization_barrier((picked(x_tokens, first), all_counts))
        x_first = exchange(x_first).reshape(n_rows, d_model)
        arriving = lax.dynamic_index_in_dim(all_counts, me, 1, keepdims=False)
        load_frac = jnp.sum(all_counts, axis=0).astype(F32) / total_tok
        dy_first, x_first = lax.optimization_barrier((picked(grad_y, first), x_first))
        dy_first = exchange(dy_first).reshape(n_rows, d_model)
        x_last, dy_first = lax.optimization_barrier((picked(x_tokens, second), dy_first))
        x_last = exchange(x_last).reshape(n_rows, d_model)
        dy_last, x_last = lax.optimization_barrier((picked(grad_y, second), x_last))
        dy_last = exchange(dy_last).reshape(n_rows, d_model)

        prob, log_norm = router(x_tokens, w_router)
        gate = jnp.sum(prob * hot_f, axis=-1)
        aux_vec = AUX_WEIGHT * num_experts * load_frac / total_tok
        spread = jnp.sum(prob * aux_vec, axis=-1, keepdims=True)
        d_logits = prob * (aux_vec - spread) + (2.0 * Z_WEIGHT / total_tok * log_norm)[:, None] * prob
        part_router = jnp.einsum('sd,se->de', x_tokens, d_logits, preferred_element_type=F32)

        mine = (jnp.arange(num_experts) == me).astype(F32)[None, :]

        def forward(j, rows, dy):
            slot_prob, _ = router(rows, w_router)
            slot_gate = jnp.sum(slot_prob * mine, axis=-1)
            hidden = jnp.maximum(jnp.dot(rows, w_in, preferred_element_type=F32), 0.0).astype(BF)
            expert_out = jnp.dot(hidden, w_out, preferred_element_type=F32).astype(BF)
            dy_f = dy.astype(F32)
            slots = j * width + jnp.arange(width, dtype=jnp.int32)
            valid = (slots[None, :] < arriving[:, None]).reshape(n_rows)
            slot_dot = jnp.where(valid, jnp.sum(expert_out.astype(F32) * dy_f, axis=-1), 0.0)
            scaled = jnp.where(valid[:, None], slot_gate[:, None] * dy_f, 0.0).astype(BF)
            slot_logits = (slot_gate * slot_dot)[:, None] * (mine - slot_prob)
            part = jnp.einsum('sd,se->de', rows, slot_logits, preferred_element_type=F32)
            return hidden, scaled, slot_dot.reshape(n_dev, width), part

        def backward(hidden, scaled):
            d_hidden = jnp.einsum('nd,fd->nf', scaled, w_out, preferred_element_type=F32)
            d_pre = jnp.where(hidden > 0, d_hidden, 0.0).astype(BF)
            d_rows = jnp.einsum('nf,df->nd', d_pre, w_in, preferred_element_type=F32).astype(BF)
            return d_pre, d_rows.reshape(n_dev, width, d_model)

        def weights(rows, hidden, scaled, d_pre):
            return (jnp.einsum('nd,nf->df', rows, d_pre, preferred_element_type=F32),
                    jnp.einsum('nf,nd->fd', hidden, scaled, preferred_element_type=F32))

        hidden_a, scaled_a, dot_a, part_a = forward(0, x_first, dy_first)
        pre_a, d_rows_a = backward(hidden_a, scaled_a)
        in_a = jnp.einsum('nd,nf->df', x_first, pre_a, preferred_element_type=F32)
        d_rows_a, in_a = lax.optimization_barrier((d_rows_a, in_a))
        back_a = exchange(d_rows_a)
        hidden_b, scaled_b, dot_b, part_b = forward(1, x_last, dy_last)
        pre_b, d_rows_b = backward(hidden_b, scaled_b)

        part_router += part_a + part_b
        slices = part_router.reshape(n_dev, -1)
        prob_sum = jnp.sum(prob, axis=0)[:, None]
        z_sum = jnp.full((n_dev, 1), jnp.sum(log_norm * log_norm))
        payload = jnp.concatenate([dot_a, dot_b, slices, prob_sum, z_sum], axis=1)
        payload, back_a, d_rows_b = lax.optimization_barrier((payload, back_a, d_rows_b))
        payload = exchange(payload)
        payload, d_rows_b = lax.optimization_barrier((payload, d_rows_b))
        back_b = exchange(d_rows_b)
        reduced = jnp.sum(payload[:, capacity:], axis=0)
        reduced, back_b = lax.optimization_barrier((reduced, back_b))
        totals = exchange(jnp.broadcast_to(reduced[None, :], (n_dev, reduced.shape[0])))
        grad_w_router = totals[:, :-2].reshape(d_model, num_experts)
        aux_loss = AUX_WEIGHT * num_experts * jnp.sum(load_frac * (totals[:, -2] / total_tok))
        z_loss = Z_WEIGHT * totals[0, -1] / total_tok

        payload, hidden_a, hidden_b, pre_b, back_a = lax.optimization_barrier((payload, hidden_a, hidden_b, pre_b, back_a))
        out_a = jnp.einsum('nf,nd->fd', hidden_a, scaled_a, preferred_element_type=F32)
        in_b, out_b = weights(x_last, hidden_b, scaled_b, pre_b)

        all_dot = payload[:, :capacity]

        def placed(j, back):
            inside = position - j * width
            index = jnp.where((inside >= 0) & (inside < width), expert_idx * width + inside, -1)
            pick = (index[:, None] == jnp.arange(n_rows, dtype=jnp.int32)[None, :]).astype(BF)
            return jnp.dot(pick, back.reshape(n_rows, d_model), preferred_element_type=F32)

        spread_dot = jnp.dot(hot_f, all_dot, precision=lax.Precision.HIGHEST, preferred_element_type=F32)
        d_gate = jnp.sum(jnp.where(pos_hot > 0, spread_dot, 0.0), axis=-1)
        d_logits += (gate * d_gate)[:, None] * (hot_f - prob)
        dx = jnp.einsum('se,de->sd', d_logits, w_router)
        dx += placed(0, back_a)
        dx, back_b = lax.optimization_barrier((dx, back_b))
        dx += placed(1, back_b)
        return dx.astype(BF), (in_a + in_b)[None], (out_a + out_b)[None], grad_w_router, aux_loss, z_loss

    return jax.shard_map(expert_layer, mesh=mesh,
                         in_specs=(P('ep', None), P(None, None), P('ep'), P('ep', None, None), P('ep', None, None), P('ep', None)),
                         out_specs=(P('ep', None), P('ep', None, None), P('ep', None, None), P(None, None), P(), P()),
                         check_vma=False)
```

```python
import functools

import jax
import jax.numpy as jnp
from jax import lax
from jax.experimental import pallas as pl
from jax.experimental.pallas import tpu as pltpu
from jax.sharding import PartitionSpec as P

AUX_WEIGHT = 0.01
Z_WEIGHT = 0.001
CHUNKS = 2
BLOCK = 256
BF = jnp.bfloat16
F32 = jnp.float32


def route(idx, num_experts, capacity):
    tokens = idx.shape[0]
    hot = (idx[:, None] == jnp.arange(num_experts, dtype=jnp.int32)[None, :]).astype(BF)
    blocks = hot.reshape(tokens // BLOCK, BLOCK, num_experts)
    row = lax.broadcasted_iota(jnp.int32, (BLOCK, BLOCK), 0)
    col = lax.broadcasted_iota(jnp.int32, (BLOCK, BLOCK), 1)
    inside = jnp.einsum('ij,bje->bie', (col <= row).astype(BF), blocks, preferred_element_type=F32)
    totals = inside[:, -1, :]
    n_blocks = tokens // BLOCK
    earlier = (jnp.arange(n_blocks)[None, :] < jnp.arange(n_blocks)[:, None]).astype(F32)
    before = jnp.sum(earlier[:, :, None] * totals[None, :, :], axis=1)
    counts = (before[-1] + totals[-1]).astype(jnp.int32)
    position = jnp.sum((inside + before[:, None, :]) * blocks.astype(F32), axis=-1).reshape(tokens).astype(jnp.int32) - 1
    pos_hot = (position[:, None] == jnp.arange(capacity, dtype=jnp.int32)[None, :]).astype(BF)
    token = jnp.arange(tokens, dtype=jnp.int32)
    parts = jnp.concatenate([hot * (token // 64).astype(BF)[:, None], hot * (token % 64).astype(BF)[:, None]], axis=1)
    found = jnp.einsum('te,tp->ep', parts, pos_hot, preferred_element_type=F32)
    slot_tok = (64.0 * found[:num_experts] + found[num_experts:]).astype(jnp.int32)
    return hot, pos_hot, counts, position, slot_tok


GROUP = 4
DEPTH = 1024


def first_exchange(n_dev, width, slot_ref, x_ref, dy_ref, x_got, dy_got, x_late, dy_late, stage, total,
                   send_sem, recv_sem, own_sem, late_sem):
    me = lax.axis_index('ep')
    tokens = x_ref.shape[0]
    rows = GROUP * width
    n_groups = n_dev // GROUP
    got = (x_got, dy_got)
    late = (x_late, dy_late)
    block = lambda first, count: pl.ds(pl.multiple_of(first * width, 8), count * width)

    def group_of(i):
        return lax.rem(me // GROUP + n_groups // 2 + i, n_groups)

    def fill(k, i):
        group = group_of(i)
        index = slot_ref[k // 2, block(group * GROUP, GROUP), :]
        source = (x_ref, dy_ref)[k % 2]
        total[...] = jnp.zeros_like(total)

        def add(j, carry):
            first = j * DEPTH
            token = lax.broadcasted_iota(jnp.int32, (rows, DEPTH), 1) + first
            pick = jnp.where(token == index, 1.0, 0.0).astype(BF)
            total[...] += jnp.dot(pick, source[pl.ds(pl.multiple_of(first, DEPTH), DEPTH), :], preferred_element_type=F32)
            return carry

        lax.fori_loop(0, tokens // DEPTH, add, 0)
        stage[k, block(group * GROUP, GROUP), :] = total[...].astype(BF)

    def send(k, i):
        group = group_of(i)
        if k >= 2:
            where = block(group * GROUP, GROUP)
            pltpu.make_async_copy(stage.at[k, where], late[k - 2].at[where], late_sem.at[k - 2]).start()
            return
        for j in range(GROUP):
            peer = group * GROUP + j
            source = stage.at[k, block(peer, 1)]
            target = got[k].at[block(me, 1)]

            @pl.when(peer != me)
            def _():
                pltpu.make_async_remote_copy(source, target, send_sem.at[k], recv_sem.at[k], device_id=(peer,),
                                             device_id_type=pl.DeviceIdType.MESH).start()

            @pl.when(peer == me)
            def _():
                pltpu.make_async_copy(source, target, own_sem.at[k]).start()

    for k in range(4):
        fill(k, 0)
        if k > 0:
            send(k - 1, n_groups - 1)

        def step(i, carry, k=k):
            fill(k, i)
            send(k, i - 1)
            return carry

        lax.fori_loop(1, n_groups, step, 0)
    send(3, n_groups - 1)
    for k in range(2):
        others = got[k].at[block(0, n_dev - 1)]
        pltpu.make_async_copy(stage.at[k + 2], late[k], late_sem.at[k]).wait()
        pltpu.make_async_copy(stage.at[k, block(0, 1)], got[k].at[block(0, 1)], own_sem.at[k]).wait()
        pltpu.make_async_copy(others, others, send_sem.at[k]).wait()
        pltpu.make_async_copy(others, others, recv_sem.at[k]).wait()


def start_rows(n_dev, slot_tok, x_tokens, grad_y):
    width = slot_tok.shape[1] // CHUNKS
    tokens, d_model = x_tokens.shape
    n_rows = n_dev * width
    slots = slot_tok.reshape(n_dev, CHUNKS, width).transpose(1, 0, 2).reshape(CHUNKS, n_rows, 1)
    vmem = pl.BlockSpec(memory_space=pltpu.VMEM)
    hbm = pl.BlockSpec(memory_space=pl.ANY)
    out = jax.ShapeDtypeStruct((n_rows, d_model), BF)
    return pl.pallas_call(
        functools.partial(first_exchange, n_dev, width),
        out_shape=[out] * 4,
        in_specs=[vmem] * 3,
        out_specs=[hbm] * 4,
        scratch_shapes=[
            pltpu.VMEM((4, n_rows, d_model), BF),
            pltpu.VMEM((GROUP * width, d_model), F32),
            pltpu.SemaphoreType.DMA((2,)),
            pltpu.SemaphoreType.DMA((2,)),
            pltpu.SemaphoreType.DMA((2,)),
            pltpu.SemaphoreType.DMA((2,)),
        ],
        compiler_params=pltpu.CompilerParams(has_side_effects=True, vmem_limit_bytes=60 * 2 ** 20),
        cost_estimate=pl.CostEstimate(flops=8 * n_rows * tokens * d_model, bytes_accessed=40 * 2 ** 20, transcendentals=0),
    )(slots, x_tokens, grad_y)


def router(rows, w_router):
    logits = jnp.dot(rows, w_router, preferred_element_type=F32)
    return jax.nn.softmax(logits, axis=-1), jax.nn.logsumexp(logits, axis=-1)


def solution(mesh):
    n_dev = mesh.shape['ep']

    def expert_layer(x_tokens, w_router, expert_idx, w_in, w_out, grad_y):
        tokens, d_model = x_tokens.shape
        num_experts = n_dev
        capacity = (5 * tokens + 4 * num_experts - 1) // (4 * num_experts)
        total_tok = tokens * n_dev
        width = capacity // CHUNKS
        me = lax.axis_index('ep')
        w_in, w_out = w_in[0], w_out[0]

        def exchange(rows):
            return lax.all_to_all(rows, 'ep', 0, 0, tiled=True)

        hot, pos_hot, counts, position, slot_tok = route(expert_idx, num_experts, capacity)
        hot_f = hot.astype(F32)
        all_counts = exchange(jnp.broadcast_to(counts[None, :], (n_dev, num_experts)))

        n_rows = n_dev * width
        slot_tok, all_counts = lax.optimization_barrier((slot_tok, all_counts))
        x_first, dy_first, x_send, dy_send = start_rows(n_dev, slot_tok, x_tokens, grad_y)
        arriving = lax.dynamic_index_in_dim(all_counts, me, 1, keepdims=False)
        load_frac = jnp.sum(all_counts, axis=0).astype(F32) / total_tok
        x_last = exchange(x_send.reshape(n_dev, width, d_model)).reshape(n_rows, d_model)
        dy_send, x_last = lax.optimization_barrier((dy_send, x_last))
        dy_last = exchange(dy_send.reshape(n_dev, width, d_model)).reshape(n_rows, d_model)

        prob, log_norm = router(x_tokens, w_router)
        gate = jnp.sum(prob * hot_f, axis=-1)
        aux_vec = AUX_WEIGHT * num_experts * load_frac / total_tok
        spread = jnp.sum(prob * aux_vec, axis=-1, keepdims=True)
        d_logits = prob * (aux_vec - spread) + (2.0 * Z_WEIGHT / total_tok * log_norm)[:, None] * prob
        part_router = jnp.einsum('sd,se->de', x_tokens, d_logits, preferred_element_type=F32)

        mine = (jnp.arange(num_experts) == me).astype(F32)[None, :]

        def forward(j, rows, dy):
            slot_prob, _ = router(rows, w_router)
            slot_gate = jnp.sum(slot_prob * mine, axis=-1)
            hidden = jnp.maximum(jnp.dot(rows, w_in, preferred_element_type=F32), 0.0).astype(BF)
            expert_out = jnp.dot(hidden, w_out, preferred_element_type=F32).astype(BF)
            dy_f = dy.astype(F32)
            slots = j * width + jnp.arange(width, dtype=jnp.int32)
            valid = (slots[None, :] < arriving[:, None]).reshape(n_rows)
            slot_dot = jnp.where(valid, jnp.sum(expert_out.astype(F32) * dy_f, axis=-1), 0.0)
            scaled = jnp.where(valid[:, None], slot_gate[:, None] * dy_f, 0.0).astype(BF)
            slot_logits = (slot_gate * slot_dot)[:, None] * (mine - slot_prob)
            part = jnp.einsum('sd,se->de', rows, slot_logits, preferred_element_type=F32)
            return hidden, scaled, slot_dot.reshape(n_dev, width), part

        def backward(hidden, scaled):
            d_hidden = jnp.einsum('nd,fd->nf', scaled, w_out, preferred_element_type=F32)
            d_pre = jnp.where(hidden > 0, d_hidden, 0.0).astype(BF)
            d_rows = jnp.einsum('nf,df->nd', d_pre, w_in, preferred_element_type=F32).astype(BF)
            return d_pre, d_rows.reshape(n_dev, width, d_model)

        def weights(rows, hidden, scaled, d_pre):
            return (jnp.einsum('nd,nf->df', rows, d_pre, preferred_element_type=F32),
                    jnp.einsum('nf,nd->fd', hidden, scaled, preferred_element_type=F32))

        hidden_a, scaled_a, dot_a, part_a = forward(0, x_first, dy_first)
        pre_a, d_rows_a = backward(hidden_a, scaled_a)
        in_a = jnp.einsum('nd,nf->df', x_first, pre_a, preferred_element_type=F32)
        d_rows_a, in_a = lax.optimization_barrier((d_rows_a, in_a))
        back_a = exchange(d_rows_a)
        hidden_b, scaled_b, dot_b, part_b = forward(1, x_last, dy_last)
        pre_b, d_rows_b = backward(hidden_b, scaled_b)

        part_router += part_a + part_b
        slices = part_router.reshape(n_dev, -1)
        prob_sum = jnp.sum(prob, axis=0)[:, None]
        z_sum = jnp.full((n_dev, 1), jnp.sum(log_norm * log_norm))
        payload = jnp.concatenate([dot_a, dot_b, slices, prob_sum, z_sum], axis=1)
        payload, back_a, d_rows_b = lax.optimization_barrier((payload, back_a, d_rows_b))
        payload = exchange(payload)
        payload, d_rows_b = lax.optimization_barrier((payload, d_rows_b))
        back_b = exchange(d_rows_b)
        reduced = jnp.sum(payload[:, capacity:], axis=0)
        reduced, back_b = lax.optimization_barrier((reduced, back_b))
        totals = exchange(jnp.broadcast_to(reduced[None, :], (n_dev, reduced.shape[0])))
        grad_w_router = totals[:, :-2].reshape(d_model, num_experts)
        aux_loss = AUX_WEIGHT * num_experts * jnp.sum(load_frac * (totals[:, -2] / total_tok))
        z_loss = Z_WEIGHT * totals[0, -1] / total_tok

        payload, hidden_a, hidden_b, pre_b, back_a = lax.optimization_barrier((payload, hidden_a, hidden_b, pre_b, back_a))
        out_a = jnp.einsum('nf,nd->fd', hidden_a, scaled_a, preferred_element_type=F32)
        in_b, out_b = weights(x_last, hidden_b, scaled_b, pre_b)

        all_dot = payload[:, :capacity]

        def placed(j, back):
            inside = position - j * width
            index = jnp.where((inside >= 0) & (inside < width), expert_idx * width + inside, -1)
            pick = (index[:, None] == jnp.arange(n_rows, dtype=jnp.int32)[None, :]).astype(BF)
            return jnp.dot(pick, back.reshape(n_rows, d_model), preferred_element_type=F32)

        spread_dot = jnp.dot(hot_f, all_dot, precision=lax.Precision.HIGHEST, preferred_element_type=F32)
        d_gate = jnp.sum(jnp.where(pos_hot > 0, spread_dot, 0.0), axis=-1)
        d_logits += (gate * d_gate)[:, None] * (hot_f - prob)
        dx = jnp.einsum('se,de->sd', d_logits, w_router)
        dx += placed(0, back_a)
        dx, back_b = lax.optimization_barrier((dx, back_b))
        dx += placed(1, back_b)
        return dx.astype(BF), (in_a + in_b)[None], (out_a + out_b)[None], grad_w_router, aux_loss, z_loss

    return jax.shard_map(expert_layer, mesh=mesh,
                         in_specs=(P('ep', None), P(None, None), P('ep'), P('ep', None, None), P('ep', None, None), P('ep', None)),
                         out_specs=(P('ep', None), P('ep', None, None), P('ep', None, None), P(None, None), P(), P()),
                         check_vma=False)
```

```python
import functools

import jax
import jax.numpy as jnp
from jax import lax
from jax.experimental import pallas as pl
from jax.experimental.pallas import tpu as pltpu
from jax.sharding import PartitionSpec as P

AUX_WEIGHT = 0.01
Z_WEIGHT = 0.001
CHUNKS = 2
BLOCK = 256
BF = jnp.bfloat16
F32 = jnp.float32


def route(idx, num_experts, capacity):
    tokens = idx.shape[0]
    hot = (idx[:, None] == jnp.arange(num_experts, dtype=jnp.int32)[None, :]).astype(BF)
    blocks = hot.reshape(tokens // BLOCK, BLOCK, num_experts)
    row = lax.broadcasted_iota(jnp.int32, (BLOCK, BLOCK), 0)
    col = lax.broadcasted_iota(jnp.int32, (BLOCK, BLOCK), 1)
    inside = jnp.einsum('ij,bje->bie', (col <= row).astype(BF), blocks, preferred_element_type=F32)
    totals = inside[:, -1, :]
    n_blocks = tokens // BLOCK
    earlier = (jnp.arange(n_blocks)[None, :] < jnp.arange(n_blocks)[:, None]).astype(F32)
    before = jnp.sum(earlier[:, :, None] * totals[None, :, :], axis=1)
    counts = (before[-1] + totals[-1]).astype(jnp.int32)
    position = jnp.sum((inside + before[:, None, :]) * blocks.astype(F32), axis=-1).reshape(tokens).astype(jnp.int32) - 1
    pos_hot = (position[:, None] == jnp.arange(capacity, dtype=jnp.int32)[None, :]).astype(BF)
    token = jnp.arange(tokens, dtype=jnp.int32)
    parts = jnp.concatenate([hot * (token // 64).astype(BF)[:, None], hot * (token % 64).astype(BF)[:, None]], axis=1)
    found = jnp.einsum('te,tp->ep', parts, pos_hot, preferred_element_type=F32)
    slot_tok = (64.0 * found[:num_experts] + found[num_experts:]).astype(jnp.int32)
    return hot, pos_hot, counts, position, slot_tok


def rows_of(source, index):
    return source.at[index].get(mode='promise_in_bounds')


GROUP = 8
DEPTH = 1024


def first_exchange(n_dev, width, count_ref, slot_ref, x_ref, dy_hbm, count_got, x_got, dy_got, x_late, dy_ref, stage, total,
                   send_sem, recv_sem, own_sem, late_sem, load_sem):
    me = lax.axis_index('ep')
    load = pltpu.make_async_copy(dy_hbm, dy_ref, load_sem)
    load.start()
    tokens = x_ref.shape[0]
    rows = GROUP * width
    n_groups = n_dev // GROUP
    got = (x_got, dy_got)
    tile = count_ref.shape[0]

    def tell(k, carry):
        peer = lax.rem(me + k, n_dev)
        pltpu.make_async_remote_copy(count_ref, count_got.at[pl.ds(pl.multiple_of(me * tile, tile), tile)], send_sem.at[2], recv_sem.at[2],
                                     device_id=(peer,), device_id_type=pl.DeviceIdType.MESH).start()
        return carry

    lax.fori_loop(1, n_dev, tell, 0)
    pltpu.make_async_copy(count_ref, count_got.at[pl.ds(pl.multiple_of(me * tile, tile), tile)], own_sem.at[2]).start()
    block = lambda first, count: pl.ds(pl.multiple_of(first * width, 8), count * width)

    def group_of(i):
        return lax.rem(me // GROUP + n_groups // 2 + i, n_groups)

    def fill(k, i):
        group = group_of(i)
        index = slot_ref[k // 2, block(group * GROUP, GROUP), :]
        source = (x_ref, dy_ref)[k % 2]
        total[...] = jnp.zeros_like(total)

        def add(j, carry):
            first = j * DEPTH
            token = lax.broadcasted_iota(jnp.int32, (rows, DEPTH), 1) + first
            pick = jnp.where(token == index, 1.0, 0.0).astype(BF)
            total[...] += jnp.dot(pick, source[pl.ds(pl.multiple_of(first, DEPTH), DEPTH), :], preferred_element_type=F32)
            return carry

        lax.fori_loop(0, tokens // DEPTH, add, 0)
        stage[k, block(group * GROUP, GROUP), :] = total[...].astype(BF)

    def send(k, i):
        group = group_of(i)
        if k >= 2:
            where = block(group * GROUP, GROUP)
            pltpu.make_async_copy(stage.at[k, where], x_late.at[where], late_sem).start()
            return
        for j in range(GROUP):
            peer = group * GROUP + j
            source = stage.at[k, block(peer, 1)]
            target = got[k].at[block(me, 1)]

            @pl.when(peer != me)
            def _():
                pltpu.make_async_remote_copy(source, target, send_sem.at[k], recv_sem.at[k], device_id=(peer,),
                                             device_id_type=pl.DeviceIdType.MESH).start()

            @pl.when(peer == me)
            def _():
                pltpu.make_async_copy(source, target, own_sem.at[k]).start()

    for k in range(3):
        if k == 1:
            load.wait()
        fill(k, 0)
        if k > 0:
            send(k - 1, n_groups - 1)

        def step(i, carry, k=k):
            fill(k, i)
            send(k, i - 1)
            return carry

        lax.fori_loop(1, n_groups, step, 0)
    send(2, n_groups - 1)
    pltpu.make_async_copy(stage.at[2], x_late, late_sem).wait()
    told = count_got.at[pl.ds(0, (n_dev - 1) * tile)]
    pltpu.make_async_copy(count_ref, count_got.at[pl.ds(0, tile)], own_sem.at[2]).wait()
    pltpu.make_async_copy(told, told, send_sem.at[2]).wait()
    pltpu.make_async_copy(told, told, recv_sem.at[2]).wait()
    for k in range(2):
        others = got[k].at[block(0, n_dev - 1)]
        pltpu.make_async_copy(stage.at[k, block(0, 1)], got[k].at[block(0, 1)], own_sem.at[k]).wait()
        pltpu.make_async_copy(others, others, send_sem.at[k]).wait()
        pltpu.make_async_copy(others, others, recv_sem.at[k]).wait()


def start_rows(n_dev, counts, slot_tok, x_tokens, grad_y):
    width = slot_tok.shape[1] // CHUNKS
    tokens, d_model = x_tokens.shape
    n_rows = n_dev * width
    slots = slot_tok.reshape(n_dev, CHUNKS, width).transpose(1, 0, 2).reshape(CHUNKS, n_rows, 1)
    vmem = pl.BlockSpec(memory_space=pltpu.VMEM)
    hbm = pl.BlockSpec(memory_space=pl.ANY)
    out = jax.ShapeDtypeStruct((n_rows, d_model), BF)
    block = jnp.pad(counts[None, :], ((0, 7), (0, 128 - counts.shape[0])))
    return pl.pallas_call(
        functools.partial(first_exchange, n_dev, width),
        out_shape=[jax.ShapeDtypeStruct((n_dev * 8, 128), jnp.int32)] + [out] * 3,
        in_specs=[vmem] * 3 + [hbm],
        out_specs=[hbm] * 4,
        scratch_shapes=[
            pltpu.VMEM((tokens, d_model), BF),
            pltpu.VMEM((3, n_rows, d_model), BF),
            pltpu.VMEM((GROUP * width, d_model), F32),
            pltpu.SemaphoreType.DMA((3,)),
            pltpu.SemaphoreType.DMA((3,)),
            pltpu.SemaphoreType.DMA((3,)),
            pltpu.SemaphoreType.DMA,
            pltpu.SemaphoreType.DMA,
        ],
        compiler_params=pltpu.CompilerParams(has_side_effects=True, vmem_limit_bytes=60 * 2 ** 20),
        cost_estimate=pl.CostEstimate(flops=6 * n_rows * tokens * d_model, bytes_accessed=40 * 2 ** 20, transcendentals=0),
    )(block, slots, x_tokens, grad_y)


def router(rows, w_router):
    logits = jnp.dot(rows, w_router, preferred_element_type=F32)
    return jax.nn.softmax(logits, axis=-1), jax.nn.logsumexp(logits, axis=-1)


def solution(mesh):
    n_dev = mesh.shape['ep']

    def expert_layer(x_tokens, w_router, expert_idx, w_in, w_out, grad_y):
        tokens, d_model = x_tokens.shape
        num_experts = n_dev
        capacity = (5 * tokens + 4 * num_experts - 1) // (4 * num_experts)
        total_tok = tokens * n_dev
        width = capacity // CHUNKS
        me = lax.axis_index('ep')
        w_in, w_out = w_in[0], w_out[0]

        def exchange(rows):
            return lax.all_to_all(rows, 'ep', 0, 0, tiled=True)

        hot, pos_hot, counts, position, slot_tok = route(expert_idx, num_experts, capacity)
        hot_f = hot.astype(F32)

        n_rows = n_dev * width
        count_got, x_first, dy_first, x_send = start_rows(n_dev, counts, slot_tok, x_tokens, grad_y)
        all_counts = count_got.reshape(n_dev, 8, 128)[:, 0, :num_experts]
        arriving = lax.dynamic_index_in_dim(all_counts, me, 1, keepdims=False)
        load_frac = jnp.sum(all_counts, axis=0).astype(F32) / total_tok
        x_last = exchange(x_send.reshape(n_dev, width, d_model)).reshape(n_rows, d_model)
        late, count_got = lax.optimization_barrier((slot_tok[:, width:].reshape(-1), count_got))
        dy_send = rows_of(grad_y, late)
        dy_send, x_last = lax.optimization_barrier((dy_send, x_last))
        dy_last = exchange(dy_send.reshape(n_dev, width, d_model)).reshape(n_rows, d_model)

        prob, log_norm = router(x_tokens, w_router)
        gate = jnp.sum(prob * hot_f, axis=-1)
        aux_vec = AUX_WEIGHT * num_experts * load_frac / total_tok
        spread = jnp.sum(prob * aux_vec, axis=-1, keepdims=True)
        d_logits = prob * (aux_vec - spread) + (2.0 * Z_WEIGHT / total_tok * log_norm)[:, None] * prob
        part_router = jnp.einsum('sd,se->de', x_tokens, d_logits, preferred_element_type=F32)

        mine = (jnp.arange(num_experts) == me).astype(F32)[None, :]

        def forward(j, rows, dy):
            slot_prob, _ = router(rows, w_router)
            slot_gate = jnp.sum(slot_prob * mine, axis=-1)
            hidden = jnp.maximum(jnp.dot(rows, w_in, preferred_element_type=F32), 0.0).astype(BF)
            expert_out = jnp.dot(hidden, w_out, preferred_element_type=F32).astype(BF)
            dy_f = dy.astype(F32)
            slots = j * width + jnp.arange(width, dtype=jnp.int32)
            valid = (slots[None, :] < arriving[:, None]).reshape(n_rows)
            slot_dot = jnp.where(valid, jnp.sum(expert_out.astype(F32) * dy_f, axis=-1), 0.0)
            scaled = jnp.where(valid[:, None], slot_gate[:, None] * dy_f, 0.0).astype(BF)
            slot_logits = (slot_gate * slot_dot)[:, None] * (mine - slot_prob)
            part = jnp.einsum('sd,se->de', rows, slot_logits, preferred_element_type=F32)
            return hidden, scaled, slot_dot.reshape(n_dev, width), part

        def backward(hidden, scaled):
            d_hidden = jnp.einsum('nd,fd->nf', scaled, w_out, preferred_element_type=F32)
            d_pre = jnp.where(hidden > 0, d_hidden, 0.0).astype(BF)
            d_rows = jnp.einsum('nf,df->nd', d_pre, w_in, preferred_element_type=F32).astype(BF)
            return d_pre, d_rows.reshape(n_dev, width, d_model)

        def weights(rows, hidden, scaled, d_pre):
            return (jnp.einsum('nd,nf->df', rows, d_pre, preferred_element_type=F32),
                    jnp.einsum('nf,nd->fd', hidden, scaled, preferred_element_type=F32))

        hidden_a, scaled_a, dot_a, part_a = forward(0, x_first, dy_first)
        pre_a, d_rows_a = backward(hidden_a, scaled_a)
        in_a = jnp.einsum('nd,nf->df', x_first, pre_a, preferred_element_type=F32)
        d_rows_a, in_a = lax.optimization_barrier((d_rows_a, in_a))
        back_a = exchange(d_rows_a)
        hidden_b, scaled_b, dot_b, part_b = forward(1, x_last, dy_last)
        pre_b, d_rows_b = backward(hidden_b, scaled_b)

        part_router += part_a + part_b
        slices = part_router.reshape(n_dev, -1)
        prob_sum = jnp.sum(prob, axis=0)[:, None]
        z_sum = jnp.full((n_dev, 1), jnp.sum(log_norm * log_norm))
        payload = jnp.concatenate([dot_a, dot_b, slices, prob_sum, z_sum], axis=1)
        payload, back_a, d_rows_b = lax.optimization_barrier((payload, back_a, d_rows_b))
        payload = exchange(payload)
        payload, d_rows_b = lax.optimization_barrier((payload, d_rows_b))
        back_b = exchange(d_rows_b)
        reduced = jnp.sum(payload[:, capacity:], axis=0)
        reduced, back_b = lax.optimization_barrier((reduced, back_b))
        totals = exchange(jnp.broadcast_to(reduced[None, :], (n_dev, reduced.shape[0])))
        grad_w_router = totals[:, :-2].reshape(d_model, num_experts)
        aux_loss = AUX_WEIGHT * num_experts * jnp.sum(load_frac * (totals[:, -2] / total_tok))
        z_loss = Z_WEIGHT * totals[0, -1] / total_tok

        payload, hidden_a, hidden_b, pre_b, back_a = lax.optimization_barrier((payload, hidden_a, hidden_b, pre_b, back_a))
        out_a = jnp.einsum('nf,nd->fd', hidden_a, scaled_a, preferred_element_type=F32)
        in_b, out_b = weights(x_last, hidden_b, scaled_b, pre_b)

        all_dot = payload[:, :capacity]

        def placed(j, back):
            inside = position - j * width
            index = jnp.where((inside >= 0) & (inside < width), expert_idx * width + inside, -1)
            pick = (index[:, None] == jnp.arange(n_rows, dtype=jnp.int32)[None, :]).astype(BF)
            return jnp.dot(pick, back.reshape(n_rows, d_model), preferred_element_type=F32)

        spread_dot = jnp.dot(hot_f, all_dot, precision=lax.Precision.HIGHEST, preferred_element_type=F32)
        d_gate = jnp.sum(jnp.where(pos_hot > 0, spread_dot, 0.0), axis=-1)
        d_logits += (gate * d_gate)[:, None] * (hot_f - prob)
        dx = jnp.einsum('se,de->sd', d_logits, w_router)
        dx += placed(0, back_a)
        dx, back_b = lax.optimization_barrier((dx, back_b))
        dx += placed(1, back_b)
        return dx.astype(BF), (in_a + in_b)[None], (out_a + out_b)[None], grad_w_router, aux_loss, z_loss

    return jax.shard_map(expert_layer, mesh=mesh,
                         in_specs=(P('ep', None), P(None, None), P('ep'), P('ep', None, None), P('ep', None, None), P('ep', None)),
                         out_specs=(P('ep', None), P('ep', None, None), P('ep', None, None), P(None, None), P(), P()),
                         check_vma=False)
```
